32 devices in a mesh: data: 32 (over z, y, x, core).
Axes of the slice: x: 2, y: 2, z: 4, core: 2. Of those that a mesh axis runs over, the one named last changes fastest.
Arguments:
- x_in: bfloat16 [16384, 1280], P('data')
- dy_in: bfloat16 [16384, 1280], P('data')
- weights: bfloat16 [4, 1280, 1280], replicated
- a_old: float32 [5120, 1280], P('data')
- s_old: float32 [5120, 1280], P('data')
- a_inv: float32 [5120, 1280], P('data')
- s_inv: float32 [4, 1280, 1280], replicated
Outputs:
- output 1: float32 [4, 1280, 1280], replicated
- output 2: float32 [5120, 1280], P('data')
- output 3: float32 [5120, 1280], P('data')
All inputs are finite; a program needn't handle non-finite values.
Results may differ from the reference program's by a relative error of at most 0.00156141.
Values are sent between devices in bfloat16 or wider.
A program may use at most 1 GiB of HBM per device.

```python
import functools
import jax
import jax.numpy as jnp

D = 1280
LAYERS = 4
TOKENS = 512
SHARDS = 32
LOW_RANK = 64
BATCH_TOTAL = TOKENS * SHARDS
FACTOR_DECAY = 0.75


def spd_stack(rng_key, base_diag, gram_scale):
    low_rank = jax.random.normal(rng_key, (LAYERS, D, LOW_RANK), jnp.float32)
    gram_mat = jnp.einsum("lir,ljr->lij", low_rank, low_rank)
    gram_mat = 0.5 * (gram_mat + jnp.swapaxes(gram_mat, 1, 2))
    return gram_scale * gram_mat + base_diag * jnp.eye(D, dtype=jnp.float32)


def shard_rows(rng_key, spread):
    key_raw, key_mean, key_scale = jax.random.split(rng_key, 3)
    raw_rows = jax.random.normal(key_raw, (SHARDS, TOKENS, D), jnp.float32)
    offset = 0.7 * jax.random.normal(key_mean, (SHARDS, 1, D), jnp.float32)
    row_scale = jnp.exp(spread * jax.random.normal(key_scale, (SHARDS, 1, 1), jnp.float32))
    return ((raw_rows + offset) * row_scale).reshape(BATCH_TOTAL, D).astype(jnp.bfloat16)


def setup_inputs(seed: int = 0) -> dict:
    key_list = jax.random.split(jax.random.key(seed), 7)
    weights = jax.random.normal(key_list[2], (LAYERS, D, D), jnp.float32) * D ** -0.5
    inv_scale = (LOW_RANK * D) ** -0.5
    return {
        "x_in": shard_rows(key_list[0], 0.5),
        "dy_in": shard_rows(key_list[1], 0.5),
        "weights": weights.astype(jnp.bfloat16),
        "a_old": spd_stack(key_list[3], 0.5, 1.0 / LOW_RANK).reshape(LAYERS * D, D),
        "s_old": spd_stack(key_list[4], 0.5, 1.0 / LOW_RANK).reshape(LAYERS * D, D),
        "a_inv": spd_stack(key_list[5], 0.5, inv_scale).reshape(LAYERS * D, D),
        "s_inv": spd_stack(key_list[6], 0.5, inv_scale),
    }


def gelu_grad(pre_act, d_act):
    pullback = jax.vjp(functools.partial(jax.nn.gelu, approximate=True), pre_act.astype(jnp.float32))[1]
    return pullback(d_act.astype(jnp.float32))[0].astype(jnp.bfloat16)


def reference(x_in, dy_in, weights, a_old, s_old, a_inv, s_inv):
    layer_inputs = [x_in]
    pre_acts = []
    for layer_id in range(LAYERS - 1):
        pre_act = jnp.dot(layer_inputs[layer_id], weights[layer_id], preferred_element_type=jnp.float32).astype(jnp.bfloat16)
        pre_acts.append(pre_act)
        layer_inputs.append(jax.nn.gelu(pre_act.astype(jnp.float32), approximate=True).astype(jnp.bfloat16))
    out_grads = [dy_in] * LAYERS
    for layer_id in range(LAYERS - 1, 0, -1):
        d_act = jnp.dot(out_grads[layer_id], weights[layer_id].T, preferred_element_type=jnp.float32).astype(jnp.bfloat16)
        out_grads[layer_id - 1] = gelu_grad(pre_acts[layer_id - 1], d_act)
    a_facs = []
    s_facs = []
    updates = []
    for layer_id in range(LAYERS):
        h_in = layer_inputs[layer_id]
        g_out = out_grads[layer_id]
        a_facs.append(jnp.dot(h_in.T, h_in, preferred_element_type=jnp.float32) / BATCH_TOTAL)
        s_facs.append(jnp.dot(g_out.T, g_out, preferred_element_type=jnp.float32) / BATCH_TOTAL)
        w_grad = jnp.dot(h_in.T, g_out, preferred_element_type=jnp.float32) / BATCH_TOTAL
        a_inv_layer = a_inv[layer_id * D:(layer_id + 1) * D]
        updates.append(jnp.dot(a_inv_layer, jnp.dot(w_grad, s_inv[layer_id])))
    a_new = FACTOR_DECAY * a_old + (1.0 - FACTOR_DECAY) * jnp.concatenate(a_facs, axis=0)
    s_new = FACTOR_DECAY * s_old + (1.0 - FACTOR_DECAY) * jnp.concatenate(s_facs, axis=0)
    return (jnp.stack(updates), a_new, s_new)
```

```python
import functools
import jax
import jax.numpy as jnp
from jax import lax
from jax.sharding import PartitionSpec as P

FACTOR_DECAY = 0.75
PRECISE = lax.Precision.HIGHEST
WIRE = jnp.float16


def gelu_grad(pre_act, d_act):
    pullback = jax.vjp(functools.partial(jax.nn.gelu, approximate=True), pre_act.astype(jnp.float32))[1]
    return pullback(d_act.astype(jnp.float32))[0].astype(jnp.bfloat16)


def after(value, deps):
    return lax.optimization_barrier((value, *deps))[0]


def exponent(peak):
    return jnp.clip(jnp.floor(jnp.log2(peak)) + 2.0, -60.0, 130.0)


def solution(mesh):
    n_dev = mesh.shape["data"]

    def device_step(x_loc, dy_loc, weights, a_old_rows, s_old_rows, a_inv_rows, s_inv):
        n_layers, width, _ = weights.shape
        own = a_old_rows.shape[0]
        half = width // 2
        rows_loc = x_loc.shape[0]
        batch_total = rows_loc * n_dev
        me = lax.axis_index("data")
        core, px, py, pz = me % 2, (me // 2) % 2, (me // 4) % 2, me // 8
        place = {1: core, 2: px, 4: py}

        def swap(value, mask):
            return lax.ppermute(value, "data", [(p, p ^ mask) for p in range(n_dev)])

        def pick(value, index, axis):
            return lax.dynamic_index_in_dim(value, index, axis, keepdims=False)

        def ordered(mine, other, bit, axis):
            first = place[bit] == 0
            return jnp.stack([jnp.where(first, mine, other), jnp.where(first, other, mine)], axis=axis)

        def chip(value):
            return jnp.concatenate([value, swap(value, 1)], axis=0)

        def peak(value):
            return jnp.max(jnp.abs(value)).astype(jnp.float32)

        acts, pre, acts_chip = [x_loc], [], [chip(x_loc)]
        grads, grads_chip = [None] * n_layers, [None] * n_layers
        grads[-1], grads_chip[-1] = dy_loc, chip(dy_loc)
        for l in range(n_layers - 1):
            z = jnp.dot(acts[l], weights[l], preferred_element_type=jnp.float32).astype(jnp.bfloat16)
            pre.append(z)
            acts.append(jax.nn.gelu(z.astype(jnp.float32), approximate=True).astype(jnp.bfloat16))
            acts_chip.append(chip(acts[-1]))
        for l in range(n_layers - 1, 0, -1):
            d_act = jnp.einsum("bj,ij->bi", grads[l], weights[l], preferred_element_type=jnp.float32).astype(jnp.bfloat16)
            grads[l - 1] = gelu_grad(pre[l - 1], d_act)
            grads_chip[l - 1] = chip(grads[l - 1])

        e_h = [exponent(peak(v)) for v in acts_chip]
        e_g = [exponent(peak(v)) for v in grads_chip]
        table = lax.all_gather(jnp.stack(e_h + e_g), "data", axis=0)
        e_max = jnp.max(table, axis=0)
        sides = {"A": (0, 0), "S": (n_layers, n_layers), "G": (0, n_layers)}
        chip_rows, all_rows = 2 * rows_loc, batch_total

        def total_e(vec, kind, l):
            i, j = sides[kind]
            return jnp.clip(vec[i + l] + vec[j + l], -110.0, 126.0)

        log_chip = float(chip_rows.bit_length())
        log_all = float(all_rows.bit_length())
        mine_e = jnp.stack(e_h + e_g)

        def product(kind, l):
            left = grads_chip[l] if kind == "S" else acts_chip[l]
            right = acts_chip[l] if kind == "A" else grads_chip[l]
            right = lax.dynamic_slice_in_dim(right, core * half, half, axis=1)
            out = lax.dot_general(left, right, (((0,), (0,)), ((), ())), preferred_element_type=jnp.float32)
            return out.reshape(2, 2, 2, own, half)

        def first_send(kind, l, out):
            axis, bit = (1, 2) if l % 2 == 0 else (0, 4)
            scale = jnp.exp2(15.0 - log_chip - total_e(mine_e, kind, l))
            return (pick(out, 1 - place[bit], axis) * scale).astype(WIRE)

        def first_sum(kind, l, out, got):
            axis, bit = (1, 2) if l % 2 == 0 else (0, 4)
            peer = lax.dynamic_index_in_dim(table, me ^ bit, 0, keepdims=False)
            e_peer, e_all = total_e(peer, kind, l), total_e(e_max, kind, l)
            scale = jnp.exp2(15.0 - log_all - e_all)
            ratio = jnp.exp2(jnp.clip(log_chip - log_all + e_peer - e_all, -120.0, 0.0))
            return pick(out, place[bit], axis) * scale + got.astype(jnp.float32) * ratio

        def second_bit(l):
            return 4 if l % 2 == 0 else 2

        def second_send(l, part):
            return pick(part, 1 - place[second_bit(l)], 0).astype(WIRE)

        def second_sum(l, part, got):
            return pick(part, place[second_bit(l)], 0) + got.astype(jnp.float32)

        def z_sends(parts):
            stack = jnp.stack(parts)
            return [pick(stack, pz ^ k, 0).astype(WIRE) for k in range(1, n_layers)], pick(stack, pz, 0)

        outs = {}
        early = [("A", 0), ("S", 3), ("A", 1), ("A", 2)]
        sent = {}

        def start(kind, l, deps=()):
            outs[kind, l] = product(kind, l)
            msg = first_send(kind, l, outs[kind, l])
            if deps:
                msg = after(msg, deps)
            sent[kind, l] = swap(msg, 2 if l % 2 == 0 else 4)
            return msg

        for kind, l in early:
            start(kind, l)
        for l in range(n_layers - 1, -1, -1):
            start("G", l)
        g_first = [first_sum("G", l, outs["G", l], sent["G", l]) for l in range(n_layers)]
        g_msgs = [second_send(l, g_first[l]) for l in range(n_layers)]
        g_second = [second_sum(l, g_first[l], swap(g_msgs[l], second_bit(l))) for l in range(n_layers)]

        late = [(k, l) for l in range(n_layers - 1, -1, -1) for k in ("A", "S") if (k, l) not in early]
        for kind, l in late:
            start(kind, l, g_msgs)

        sends, g_own = z_sends(g_second)
        for k, msg in enumerate(sends, 1):
            g_own = g_own + swap(msg, 8 * k).astype(jnp.float32)
        g_wire = g_own.astype(WIRE)
        g_x = ordered(g_wire, swap(g_wire, 2), 2, 0)
        g_y = ordered(g_x, swap(g_x, 4), 4, 0).reshape(width, half)
        other = swap(g_y, 1)
        g_full = jnp.where(core == 0, jnp.concatenate([g_y, other], axis=1), jnp.concatenate([other, g_y], axis=1))
        e_layer = jnp.stack([total_e(e_max, "G", l) for l in range(n_layers)])
        back = jnp.exp2(lax.dynamic_index_in_dim(e_layer, pz, 0, keepdims=False) + log_all - 15.0) / batch_total
        g_full = g_full.astype(jnp.float32) * back
        left = jnp.dot(a_inv_rows, g_full, precision=PRECISE)
        u_rows = jnp.dot(left, pick(s_inv, pz, 0), precision=PRECISE)

        new = {}
        for kind, old in (("A", a_old_rows), ("S", s_old_rows)):
            firsts = [first_sum(kind, l, outs[kind, l], sent[kind, l]) for l in range(n_layers)]
            seconds = []
            for l in range(n_layers):
                msg = after(second_send(l, firsts[l]), (g_x,))
                seconds.append(second_sum(l, firsts[l], swap(msg, second_bit(l))))
            sends, total = z_sends(seconds)
            for k, msg in enumerate(sends, 1):
                total = total + swap(msg, 8 * k).astype(jnp.float32)
            got = swap(pick(total, 1 - core, 0), 1)
            keep = pick(total, core, 0)
            rows = jnp.where(core == 0, jnp.concatenate([keep, got], axis=1), jnp.concatenate([got, keep], axis=1))
            e_layer = jnp.stack([total_e(e_max, kind, l) for l in range(n_layers)])
            back = jnp.exp2(lax.dynamic_index_in_dim(e_layer, pz, 0, keepdims=False) + log_all - 15.0)
            new[kind] = FACTOR_DECAY * old + ((1.0 - FACTOR_DECAY) / batch_total) * (rows * back)

        e_u = exponent(peak(u_rows))
        u_wire = (u_rows * jnp.exp2(14.0 - e_u)).astype(WIRE)
        e_u_all = lax.all_gather(e_u, "data", axis=0).reshape(n_layers, 2, 2, 2, 1, 1)
        u_full = jnp.zeros((n_layers, 2, 2, 2, own, width), jnp.float32)
        pieces = [u_wire] + [swap(u_wire, 8 * k) for k in range(1, n_layers)]
        for k, piece in enumerate(pieces):
            if k % 2 == 0:
                pair = ordered(piece, swap(piece, 2), 2, 0)
                quad = ordered(pair, swap(pair, 4), 4, 0)
            else:
                pair = ordered(piece, swap(piece, 4), 4, 0)
                quad = ordered(pair, swap(pair, 2), 2, 1)
            octet = ordered(quad, swap(quad, 1), 1, 2)
            e_here = pick(e_u_all, pz ^ k, 0)
            octet = octet.astype(jnp.float32) * jnp.exp2(e_here - 14.0)
            u_full = lax.dynamic_update_index_in_dim(u_full, octet, pz ^ k, 0)
        return u_full.reshape(n_layers, width, width), new["A"], new["S"]

    row_spec = P("data", None)
    return jax.shard_map(
        device_step,
        mesh=mesh,
        in_specs=(row_spec, row_spec, P(), row_spec, row_spec, row_spec, P()),
        out_specs=(P(), row_spec, row_spec),
        check_vma=False,
    )
```

```python
import functools
import jax
import jax.numpy as jnp
from jax import lax
from jax.experimental import pallas as pl
from jax.experimental.pallas import tpu as pltpu
from jax.sharding import PartitionSpec as P

MESH = pl.DeviceIdType.MESH

FACTOR_DECAY = 0.75
PRECISE = lax.Precision.HIGHEST
WIRE = jnp.float16


def gelu_grad(pre_act, d_act):
    pullback = jax.vjp(functools.partial(jax.nn.gelu, approximate=True), pre_act.astype(jnp.float32))[1]
    return pullback(d_act.astype(jnp.float32))[0].astype(jnp.bfloat16)


def after(value, deps):
    return lax.optimization_barrier((value, *deps))[0]


def fifth_power(value):
    square = value * value
    return square * square * value


def fifth_root(power):
    root = jnp.exp2(jnp.log2(jnp.abs(power)) * 0.2)
    return jnp.where(power < 0, -root, root)


def exponent(peak):
    return jnp.clip(jnp.floor(jnp.log2(peak)) + 2.0, -60.0, 130.0)


def flip(device, bit):
    return device + bit * (1 - 2 * ((device // bit) % 2))


def enter(n_dev, me):
    barrier = pltpu.get_barrier_semaphore()

    def signal(i, carry):
        pl.semaphore_signal(barrier, inc=1, device_id=(lax.rem(me + i, n_dev),), device_id_type=MESH)
        return carry

    lax.fori_loop(1, n_dev, signal, 0)
    pl.semaphore_wait(barrier, n_dev - 1)


def share(n_dev, me, mine, table, send_sem, recv_sem):
    def copy_to(i):
        peer = lax.rem(me + i, n_dev)
        return pltpu.make_async_remote_copy(
            mine, table.at[me], send_sem.at[i], recv_sem.at[i], device_id=(peer,), device_id_type=MESH
        )

    def start(i, carry):
        copy_to(i).start()
        return carry

    def wait(i, carry):
        copy_to(i).wait_send()
        source = lax.rem(me + n_dev - i, n_dev)
        pltpu.make_async_remote_copy(
            mine, table.at[source], send_sem.at[i], recv_sem.at[i], device_id=(source,), device_id_type=MESH
        ).wait_recv()
        return carry

    lax.fori_loop(1, n_dev, start, 0)
    return lambda: lax.fori_loop(1, n_dev, wait, 0)


def table_kernel(n_dev, mine, table, send_sem, recv_sem, own_sem):
    me = lax.axis_index("data")
    own = pltpu.make_async_copy(mine, table.at[me], own_sem)
    own.start()
    enter(n_dev, me)
    share(n_dev, me, mine, table, send_sem, recv_sem)()
    own.wait()


def gather_table(mine, n_dev):
    return pl.pallas_call(
        functools.partial(table_kernel, n_dev),
        out_shape=jax.ShapeDtypeStruct((n_dev, *mine.shape), mine.dtype),
        in_specs=[pl.BlockSpec(memory_space=pltpu.VMEM)],
        out_specs=pl.BlockSpec(memory_space=pl.ANY),
        scratch_shapes=[
            pltpu.SemaphoreType.DMA((n_dev,)),
            pltpu.SemaphoreType.DMA((n_dev,)),
            pltpu.SemaphoreType.DMA,
        ],
        compiler_params=pltpu.CompilerParams(collective_id=0, has_side_effects=True),
        cost_estimate=pl.CostEstimate(flops=10_000_000, bytes_accessed=300_000, transcendentals=0),
    )(mine)


def spread_kernel(n_dev, mine, scale, out, table, send_sem, recv_sem, t_send, t_recv, own_sem):
    me = lax.axis_index("data")
    own = [
        pltpu.make_async_copy(mine, out.at[me], own_sem.at[0]),
        pltpu.make_async_copy(scale, table.at[me], own_sem.at[1]),
    ]
    for copy in own:
        copy.start()
    enter(n_dev, me)
    sent = []

    def send(piece, bit, first=False):
        peer = me
        for b in bit:
            peer = flip(peer, b)
        copy = pltpu.make_async_remote_copy(
            mine if first else out.at[piece],
            out.at[piece],
            send_sem.at[len(sent)],
            recv_sem.at[piece],
            device_id=(peer,),
            device_id_type=MESH,
        )
        copy.start()
        sent.append(copy)

    def arrive(piece):
        pltpu.make_async_remote_copy(
            mine, out.at[piece], send_sem.at[0], recv_sem.at[piece], device_id=(me,), device_id_type=MESH
        ).wait_recv()

    far = {1: (8,), 2: (16,), 3: (8, 16)}

    def root(k):
        place = me
        for b in far.get(k, ()):
            place = flip(place, b)
        return place

    for k in (2, 1, 3):
        send(me, far[k], True)
    tables = share(n_dev, me, scale, table, t_send, t_recv)

    def stage(k, s):
        a, b = (2, 4) if k % 2 == 0 else (4, 2)
        p0 = root(k)
        p1 = flip(p0, a)
        p2, p3 = flip(p0, b), flip(p1, b)
        if s == 0:
            if k:
                arrive(p0)
            send(p0, (a,), k == 0)
        elif s == 1:
            arrive(p1)
            send(p0, (b,), k == 0)
            send(p1, (b,))
        elif s == 2:
            arrive(p2)
            arrive(p3)
            send(p0, (1,), k == 0)
            for p in (p1, p2, p3):
                send(p, (1,))
        else:
            for p in (p0, p1, p2, p3):
                arrive(flip(p, 1))

    order = (0, 1, 2, 3)
    for wave in range(7):
        for i, k in enumerate(order):
            if 0 <= wave - i <= 3:
                stage(k, wave - i)
    tables()
    for copy in sent:
        copy.wait_send()
    for copy in own:
        copy.wait()


def spread(mine, scale, n_dev):
    return pl.pallas_call(
        functools.partial(spread_kernel, n_dev),
        out_shape=(
            jax.ShapeDtypeStruct((n_dev, *mine.shape), mine.dtype),
            jax.ShapeDtypeStruct((n_dev, *scale.shape), scale.dtype),
        ),
        in_specs=[pl.BlockSpec(memory_space=pltpu.VMEM)] * 2,
        out_specs=(pl.BlockSpec(memory_space=pl.ANY),) * 2,
        scratch_shapes=[
            pltpu.SemaphoreType.DMA((n_dev,)),
            pltpu.SemaphoreType.DMA((n_dev,)),
            pltpu.SemaphoreType.DMA((n_dev,)),
            pltpu.SemaphoreType.DMA((n_dev,)),
            pltpu.SemaphoreType.DMA((2,)),
        ],
        compiler_params=pltpu.CompilerParams(collective_id=1, has_side_effects=True),
        cost_estimate=pl.CostEstimate(flops=100_000_000, bytes_accessed=30_000_000, transcendentals=0),
    )(mine, scale)


def solution(mesh):
    n_dev = mesh.shape["data"]

    def device_step(x_loc, dy_loc, weights, a_old_rows, s_old_rows, a_inv_rows, s_inv):
        n_layers, width, _ = weights.shape
        own = a_old_rows.shape[0]
        half = width // 2
        rows_loc = x_loc.shape[0]
        batch_total = rows_loc * n_dev
        me = lax.axis_index("data")
        core, px, py, pz = me % 2, (me // 2) % 2, (me // 4) % 2, me // 8
        place = {1: core, 2: px, 4: py}

        def swap(value, mask):
            return lax.ppermute(value, "data", [(p, p ^ mask) for p in range(n_dev)])

        def pick(value, index, axis):
            return lax.dynamic_index_in_dim(value, index, axis, keepdims=False)

        def ordered(mine, other, bit, axis):
            first = place[bit] == 0
            return jnp.stack([jnp.where(first, mine, other), jnp.where(first, other, mine)], axis=axis)

        def chip(value):
            return jnp.concatenate([value, swap(value, 1)], axis=0)

        def peak(value):
            return jnp.max(jnp.abs(value)).astype(jnp.float32)

        acts, pre, acts_chip = [x_loc], [], [chip(x_loc)]
        grads, grads_chip = [None] * n_layers, [None] * n_layers
        grads[-1], grads_chip[-1] = dy_loc, chip(dy_loc)
        settled = [(acts_chip[0],), (grads_chip[-1],)]
        for l in range(n_layers - 1):
            h_in = after(acts[l], settled.pop(0)) if l else acts[l]
            z = jnp.dot(h_in, weights[l], preferred_element_type=jnp.float32).astype(jnp.bfloat16)
            pre.append(z)
            acts.append(jax.nn.gelu(z.astype(jnp.float32), approximate=True).astype(jnp.bfloat16))
            acts_chip.append(chip(acts[-1]))
            settled.append((acts_chip[-1],))
        for l in range(n_layers - 1, 0, -1):
            g_in = after(grads[l], settled.pop(0))
            d_act = jnp.einsum("bj,ij->bi", g_in, weights[l], preferred_element_type=jnp.float32).astype(jnp.bfloat16)
            grads[l - 1] = gelu_grad(pre[l - 1], d_act)
            grads_chip[l - 1] = chip(grads[l - 1])
            settled.append((grads_chip[l - 1],))

        mine_e = jnp.stack([exponent(peak(v)) for v in acts + grads])
        table = gather_table(jnp.broadcast_to(mine_e[:, None], (2 * n_layers, 128)), n_dev)
        e_max = jnp.max(table[:, :, 0], axis=0)
        sides = {"A": (0, 0), "S": (n_layers, n_layers), "G": (0, n_layers)}

        def total_e(kind, l):
            i, j = sides[kind]
            return jnp.clip(e_max[i + l] + e_max[j + l], -110.0, 126.0)

        log_all = float(batch_total.bit_length())

        def scale_of(kind, l):
            return jnp.exp2(15.0 - log_all - total_e(kind, l))

        def unscale(kind):
            e_layer = jnp.stack([total_e(kind, l) for l in range(n_layers)])
            return jnp.exp2(lax.dynamic_index_in_dim(e_layer, pz, 0, keepdims=False) + log_all - 15.0)

        def product(kind, l, deps=()):
            left = grads_chip[l] if kind == "S" else acts_chip[l]
            right = acts_chip[l] if kind == "A" else grads_chip[l]
            if deps:
                left = after(left, deps)
            right = lax.dynamic_slice_in_dim(right, core * half, half, axis=1)
            out = lax.dot_general(left, right, (((0,), (0,)), ((), ())), preferred_element_type=jnp.float32)
            return out.reshape(2, 2, 2, own, half)

        def first_send(kind, l, out):
            axis, bit = (1, 2) if l % 2 == 0 else (0, 4)
            return (pick(out, 1 - place[bit], axis) * scale_of(kind, l)).astype(WIRE)

        def first_sum(kind, l, out, got):
            axis, bit = (1, 2) if l % 2 == 0 else (0, 4)
            return pick(out, place[bit], axis) * scale_of(kind, l) + got.astype(jnp.float32)

        def second_bit(l):
            return 4 if l % 2 == 0 else 2

        def second_send(l, part):
            return pick(part, 1 - place[second_bit(l)], 0).astype(WIRE)

        def second_sum(l, part, got):
            return pick(part, place[second_bit(l)], 0) + got.astype(jnp.float32)

        def z_sends(parts):
            stack = jnp.stack(parts)
            return [pick(stack, pz ^ k, 0).astype(WIRE) for k in range(1, n_layers)], pick(stack, pz, 0)

        outs, sent = {}, {}
        layers = range(n_layers)
        back_order = list(layers)[::-1]

        def start(kind, l, msg, deps=()):
            if deps:
                msg = after(msg, deps)
            sent[kind, l] = swap(msg, 2 if l % 2 == 0 else 4)

        g_out = {}
        for l in back_order:
            outs["G", l] = product("G", l)
            g_out[l] = first_send("G", l, outs["G", l])
            start("G", l, g_out[l])
        g_first = [first_sum("G", l, outs["G", l], sent["G", l]) for l in layers]
        g_msgs = [second_send(l, g_first[l]) for l in layers]
        g_second = [second_sum(l, g_first[l], swap(g_msgs[l], second_bit(l))) for l in layers]

        prev = tuple(g_out.values())
        for l in layers:
            outs["A", l] = product("A", l, prev)
            msg = first_send("A", l, outs["A", l])
            prev = (msg,)
            start("A", l, msg, g_msgs)

        sends, g_own = z_sends(g_second)
        for k, msg in enumerate(sends, 1):
            g_own = g_own + swap(msg, 8 * k).astype(jnp.float32)
        g_wire = g_own.astype(WIRE)
        g_x = ordered(g_wire, swap(g_wire, 2), 2, 0)
        g_y = ordered(g_x, swap(g_x, 4), 4, 0).reshape(width, half)
        other = swap(g_y, 1)
        g_full = jnp.where(core == 0, jnp.concatenate([g_y, other], axis=1), jnp.concatenate([other, g_y], axis=1))
        g_full = after(g_full.astype(jnp.float32) * (unscale("G") / batch_total), ())
        left = jnp.dot(a_inv_rows, g_full, precision=PRECISE)
        u_rows = jnp.dot(after(left, ()), pick(s_inv, pz, 0), precision=PRECISE)

        def second_stage(kind, deps):
            firsts = [first_sum(kind, l, outs[kind, l], sent[kind, l]) for l in layers]
            msgs = [after(second_send(l, firsts[l]), deps) if deps else second_send(l, firsts[l]) for l in layers]
            return firsts, msgs

        def third_stage(firsts, msgs):
            return z_sends([second_sum(l, firsts[l], swap(msgs[l], second_bit(l))) for l in layers])

        def finish(kind, old, sends, total):
            for k, msg in enumerate(sends, 1):
                total = total + swap(msg, 8 * k).astype(jnp.float32)
            got = swap(pick(total, 1 - core, 0), 1)
            keep = pick(total, core, 0)
            rows = jnp.where(core == 0, jnp.concatenate([keep, got], axis=1), jnp.concatenate([got, keep], axis=1))
            return FACTOR_DECAY * old + ((1.0 - FACTOR_DECAY) / batch_total) * (rows * unscale(kind))

        a_first, a_msgs = second_stage("A", (g_x,))
        for l in back_order:
            outs["S", l] = product("S", l, prev)
            msg = first_send("S", l, outs["S", l])
            prev = (msg,)
            start("S", l, msg, (g_x,))
        s_first, s_msgs = second_stage("S", ())
        a_sends, a_total = third_stage(a_first, a_msgs)
        a_new = finish("A", a_old_rows, a_sends, a_total)
        s_sends, s_total = third_stage(s_first, s_msgs)
        s_new = finish("S", s_old_rows, s_sends, s_total)

        e_u = exponent(peak(u_rows))
        u_unit = u_rows * jnp.exp2(-e_u)
        u_wire = fifth_power(u_unit * 2.0**20).astype(jnp.bfloat16)
        u_wire = after(u_wire, (*a_sends, *s_msgs))
        u_all, e_all = spread(u_wire, jnp.broadcast_to(e_u, (8, 128)), n_dev)
        u_full = fifth_root(u_all.astype(jnp.float32)) * jnp.exp2(e_all[:, 0, 0] - 20.0)[:, None, None]
        return u_full.reshape(n_layers, width, width), a_new, s_new

    row_spec = P("data", None)
    return jax.shard_map(
        device_step,
        mesh=mesh,
        in_specs=(row_spec, row_spec, P(), row_spec, row_spec, row_spec, P()),
        out_specs=(P(), row_spec, row_spec),
        check_vma=False,
    )
```

```python
import functools
import jax
import jax.numpy as jnp
from jax import lax
from jax.experimental import pallas as pl
from jax.experimental.pallas import tpu as pltpu
from jax.sharding import PartitionSpec as P

MESH = pl.DeviceIdType.MESH

FACTOR_DECAY = 0.75
PRECISE = lax.Precision.HIGHEST
WIRE = jnp.float16


def gelu_grad(pre_act, d_act):
    pullback = jax.vjp(functools.partial(jax.nn.gelu, approximate=True), pre_act.astype(jnp.float32))[1]
    return pullback(d_act.astype(jnp.float32))[0].astype(jnp.bfloat16)


def after(value, deps):
    return lax.optimization_barrier((value, *deps))[0]


def fifth_power(value):
    square = value * value
    return square * square * value


def fifth_root(power):
    root = jnp.exp2(jnp.log2(jnp.abs(power)) * 0.2)
    return jnp.where(power < 0, -root, root)


def exponent(peak):
    return jnp.clip(jnp.floor(jnp.log2(peak)) + 2.0, -60.0, 130.0)


def flip(device, bit):
    return device + bit * (1 - 2 * ((device // bit) % 2))


def enter(n_dev, me):
    barrier = pltpu.get_barrier_semaphore()

    def signal(i, carry):
        pl.semaphore_signal(barrier, inc=1, device_id=(lax.rem(me + i, n_dev),), device_id_type=MESH)
        return carry

    lax.fori_loop(1, n_dev, signal, 0)
    pl.semaphore_wait(barrier, n_dev - 1)


def share(n_dev, me, mine, table, send_sem, recv_sem):
    def copy_to(i):
        peer = lax.rem(me + i, n_dev)
        return pltpu.make_async_remote_copy(
            mine, table.at[me], send_sem.at[i], recv_sem.at[i], device_id=(peer,), device_id_type=MESH
        )

    def start(i, carry):
        copy_to(i).start()
        return carry

    def wait(i, carry):
        copy_to(i).wait_send()
        source = lax.rem(me + n_dev - i, n_dev)
        pltpu.make_async_remote_copy(
            mine, table.at[source], send_sem.at[i], recv_sem.at[i], device_id=(source,), device_id_type=MESH
        ).wait_recv()
        return carry

    lax.fori_loop(1, n_dev, start, 0)
    return lambda: lax.fori_loop(1, n_dev, wait, 0)


def chain_kernel(n_dev, x, dy, w_hbm, *rest):
    n_layers = w_hbm.shape[0]
    outs, (table, w, acts, pre, peaks, w_sem, own_sem, send_sem, recv_sem, t_send, t_recv, t_own) = (
        rest[: 2 * n_layers],
        rest[2 * n_layers :],
    )
    rows, width = x.shape
    me = lax.axis_index("data")
    sibling = flip(me, 1)
    barrier = pltpu.get_barrier_semaphore()

    def signal(i, carry):
        pl.semaphore_signal(barrier, inc=1, device_id=(lax.rem(me + i, n_dev),), device_id_type=MESH)
        return carry

    lax.fori_loop(1, n_dev, signal, 0)
    loads = [pltpu.make_async_copy(w_hbm.at[l], w.at[l], w_sem.at[l]) for l in range(n_layers)]
    for load in loads:
        load.start()

    def note_peak(j, ref):
        def chunk(i, best):
            part = jnp.abs(ref[pl.ds(pl.multiple_of(i * 64, 64), 64), :].astype(jnp.float32))
            return jnp.maximum(best, jnp.max(part.reshape(8, 8, width), axis=0))

        best = lax.fori_loop(0, rows // 64, chunk, jnp.zeros((8, width), jnp.float32))
        best = jnp.max(best, axis=0, keepdims=True)
        folded = best[:, :128]
        for k in range(1, width // 128):
            folded = jnp.maximum(folded, best[:, 128 * k : 128 * (k + 1)])
        peaks[j : j + 1, :] = folded

    copies = []

    def publish(j, ref):
        own = pltpu.make_async_copy(ref, outs[j].at[0], own_sem.at[j])
        there = pltpu.make_async_remote_copy(
            ref, outs[j].at[1], send_sem.at[j], recv_sem.at[j], device_id=(sibling,), device_id_type=MESH
        )
        there.start()
        own.start()
        copies.append((own, there))

    tile = 256

    def forward(l, h_in):
        h_out, z_out = acts.at[l], pre.at[l]
        loads[l].wait()

        def step(t, carry):
            cols = pl.ds(pl.multiple_of(t * tile, tile), tile)
            z = jnp.dot(h_in[...], w[l, :, cols], preferred_element_type=jnp.float32).astype(jnp.bfloat16)
            z_out[:, cols] = z
            h_out[:, cols] = jax.nn.gelu(z.astype(jnp.float32), approximate=True).astype(jnp.bfloat16)
            return carry

        lax.fori_loop(0, width // tile, step, 0)

    def backward(l, g_in):
        g_out, z_in = acts.at[n_layers - 1 + l - 1], pre.at[l - 1]
        if l == n_layers - 1:
            loads[l].wait()

        def step(t, carry):
            cols = pl.ds(pl.multiple_of(t * tile, tile), tile)
            d_act = lax.dot_general(
                g_in[...], w[l, cols, :], (((1,), (1,)), ((), ())), preferred_element_type=jnp.float32
            ).astype(jnp.bfloat16)
            g_out[:, cols] = gelu_grad(z_in[:, cols], d_act)
            return carry

        lax.fori_loop(0, width // tile, step, 0)

    note_peak(0, x)
    note_peak(2 * n_layers - 1, dy)
    forward(0, x)
    pl.semaphore_wait(barrier, n_dev - 1)
    publish(0, x)
    publish(2 * n_layers - 1, dy)
    note_peak(1, acts.at[0])
    publish(1, acts.at[0])
    for l in range(1, n_layers - 1):
        forward(l, acts.at[l - 1])
        note_peak(l + 1, acts.at[l])
        publish(l + 1, acts.at[l])
    g_in = dy
    for l in range(n_layers - 1, 0, -1):
        backward(l, g_in)
        g_in = acts.at[n_layers - 1 + l - 1]
        note_peak(n_layers + l - 1, g_in)
        publish(n_layers + l - 1, g_in)
    tables = share(n_dev, me, peaks, table, t_send, t_recv)
    mine = pltpu.make_async_copy(peaks, table.at[me], t_own)
    mine.start()
    tables()
    for own, there in copies:
        there.wait()
        own.wait()
    mine.wait()


def chain(x, dy, weights, n_dev):
    n_layers, width, _ = weights.shape
    rows = x.shape[0]
    n_acts = 2 * n_layers
    any_space = pl.BlockSpec(memory_space=pl.ANY)
    dma = pltpu.SemaphoreType.DMA
    return pl.pallas_call(
        functools.partial(chain_kernel, n_dev),
        out_shape=(
            *[jax.ShapeDtypeStruct((2, rows, width), jnp.bfloat16)] * n_acts,
            jax.ShapeDtypeStruct((n_dev, n_acts, 128), jnp.float32),
        ),
        in_specs=[pl.BlockSpec(memory_space=pltpu.VMEM)] * 2 + [any_space],
        out_specs=(any_space,) * (n_acts + 1),
        scratch_shapes=[
            pltpu.VMEM((n_layers, width, width), jnp.bfloat16),
            pltpu.VMEM((2 * n_layers - 2, rows, width), jnp.bfloat16),
            pltpu.VMEM((n_layers - 1, rows, width), jnp.bfloat16),
            pltpu.VMEM((n_acts, 128), jnp.float32),
            dma((n_layers,)),
            dma((n_acts,)),
            dma((n_acts,)),
            dma((n_acts,)),
            dma((n_dev,)),
            dma((n_dev,)),
            dma,
        ],
        compiler_params=pltpu.CompilerParams(
            collective_id=0, has_side_effects=True, vmem_limit_bytes=44 * 2**20
        ),
        cost_estimate=pl.CostEstimate(flops=10 * 2**30, bytes_accessed=40_000_000, transcendentals=5_000_000),
    )(x, dy, weights)


def spread_kernel(n_dev, mine, scale, out, table, send_sem, recv_sem, t_send, t_recv, own_sem):
    me = lax.axis_index("data")
    own = [
        pltpu.make_async_copy(mine, out.at[me], own_sem.at[0]),
        pltpu.make_async_copy(scale, table.at[me], own_sem.at[1]),
    ]
    for copy in own:
        copy.start()
    enter(n_dev, me)
    sent = []
    rows = mine.shape[0]
    whole, halves = pl.ds(0, rows), (pl.ds(0, rows // 2), pl.ds(rows // 2, rows // 2))

    def send(piece, bits, part, sem, first=False):
        peer = me
        for b in bits:
            peer = flip(peer, b)
        copy = pltpu.make_async_remote_copy(
            mine.at[part] if first else out.at[piece, part],
            out.at[piece, part],
            send_sem.at[len(sent)],
            recv_sem.at[piece, sem],
            device_id=(peer,),
            device_id_type=MESH,
        )
        copy.start()
        sent.append(copy)

    def arrive(piece, part, sem):
        pltpu.make_async_remote_copy(
            mine.at[part],
            out.at[piece, part],
            send_sem.at[0],
            recv_sem.at[piece, sem],
            device_id=(me,),
            device_id_type=MESH,
        ).wait_recv()

    far = {0: (), 1: (8,), 2: (16,), 3: (8, 16)}

    def root(k):
        place = me
        for b in far[k]:
            place = flip(place, b)
        return place

    for k in (1, 2, 3):
        send(me, far[k], whole, 0, True)
    tables = share(n_dev, me, scale, table, t_send, t_recv)
    ways = ((2, 4), (4, 2))

    def stage(k, s):
        p0 = root(k)
        near = [flip(p0, 2), flip(p0, 4)]
        last = flip(near[0], 4)
        if s == 0:
            if k:
                arrive(p0, whole, 0)
            for h, (a, b) in enumerate(ways):
                send(p0, (a,), halves[h], h, k == 0)
        elif s == 1:
            for h, (a, b) in enumerate(ways):
                send(p0, (b,), halves[h], h, k == 0)
            for h, (a, b) in enumerate(ways):
                arrive(near[h], halves[h], h)
                send(near[h], (b,), halves[h], h)
        elif s == 2:
            send(p0, (1,), whole, 0, k == 0)
            for h in range(2):
                arrive(near[1 - h], halves[h], h)
            for p in near:
                send(p, (1,), whole, 0)
            for h in range(2):
                arrive(last, halves[h], h)
            send(last, (1,), whole, 0)
        else:
            for p in (p0, *near, last):
                arrive(flip(p, 1), whole, 0)

    order = "00 01 10 02 11 20 12 21 30 22 31 03 13 32 23 33"
    for step in order.split():
        stage(int(step[0]), int(step[1]))
    tables()
    for copy in sent:
        copy.wait_send()
    for copy in own:
        copy.wait()


def spread(mine, scale, n_dev):
    return pl.pallas_call(
        functools.partial(spread_kernel, n_dev),
        out_shape=(
            jax.ShapeDtypeStruct((n_dev, *mine.shape), mine.dtype),
            jax.ShapeDtypeStruct((n_dev, *scale.shape), scale.dtype),
        ),
        in_specs=[pl.BlockSpec(memory_space=pltpu.VMEM)] * 2,
        out_specs=(pl.BlockSpec(memory_space=pl.ANY),) * 2,
        scratch_shapes=[
            pltpu.SemaphoreType.DMA((48,)),
            pltpu.SemaphoreType.DMA((n_dev, 2)),
            pltpu.SemaphoreType.DMA((n_dev,)),
            pltpu.SemaphoreType.DMA((n_dev,)),
            pltpu.SemaphoreType.DMA((2,)),
        ],
        compiler_params=pltpu.CompilerParams(collective_id=1, has_side_effects=True),
        cost_estimate=pl.CostEstimate(flops=100_000_000, bytes_accessed=30_000_000, transcendentals=0),
    )(mine, scale)


def solution(mesh):
    n_dev = mesh.shape["data"]

    def device_step(x_loc, dy_loc, weights, a_old_rows, s_old_rows, a_inv_rows, s_inv):
        n_layers, width, _ = weights.shape
        own = a_old_rows.shape[0]
        half = width // 2
        rows_loc = x_loc.shape[0]
        batch_total = rows_loc * n_dev
        me = lax.axis_index("data")
        core, px, py, pz = me % 2, (me // 2) % 2, (me // 4) % 2, me // 8
        place = {1: core, 2: px, 4: py}

        def swap(value, mask):
            return lax.ppermute(value, "data", [(p, p ^ mask) for p in range(n_dev)])

        def pick(value, index, axis):
            return lax.dynamic_index_in_dim(value, index, axis, keepdims=False)

        def ordered(mine, other, bit, axis):
            first = place[bit] == 0
            return jnp.stack([jnp.where(first, mine, other), jnp.where(first, other, mine)], axis=axis)

        *chips, table = chain(x_loc, dy_loc, weights, n_dev)
        chips = [v.reshape(2 * rows_loc, width) for v in chips]
        acts_chip, grads_chip = chips[:n_layers], chips[n_layers:]
        e_max = exponent(jnp.max(table, axis=(0, 2)))
        sides = {"A": (0, 0), "S": (n_layers, n_layers), "G": (0, n_layers)}

        def total_e(kind, l):
            i, j = sides[kind]
            return jnp.clip(e_max[i + l] + e_max[j + l], -110.0, 126.0)

        log_all = float(batch_total.bit_length())

        def scale_of(kind, l):
            return jnp.exp2(15.0 - log_all - total_e(kind, l))

        def unscale(kind):
            e_layer = jnp.stack([total_e(kind, l) for l in range(n_layers)])
            return jnp.exp2(lax.dynamic_index_in_dim(e_layer, pz, 0, keepdims=False) + log_all - 15.0)

        def product(kind, l, deps=()):
            left = grads_chip[l] if kind == "S" else acts_chip[l]
            right = acts_chip[l] if kind == "A" else grads_chip[l]
            if deps:
                left = after(left, deps)
            right = lax.dynamic_slice_in_dim(right, core * half, half, axis=1)
            out = lax.dot_general(left, right, (((0,), (0,)), ((), ())), preferred_element_type=jnp.float32)
            return out.reshape(2, 2, 2, own, half)

        def first_send(kind, l, out):
            axis, bit = (1, 2) if l % 2 == 0 else (0, 4)
            return (pick(out, 1 - place[bit], axis) * scale_of(kind, l)).astype(WIRE)

        def first_sum(kind, l, out, got):
            axis, bit = (1, 2) if l % 2 == 0 else (0, 4)
            return pick(out, place[bit], axis) * scale_of(kind, l) + got.astype(jnp.float32)

        def second_bit(l):
            return 4 if l % 2 == 0 else 2

        def second_send(l, part):
            return pick(part, 1 - place[second_bit(l)], 0).astype(WIRE)

        def second_sum(l, part, got):
            return pick(part, place[second_bit(l)], 0) + got.astype(jnp.float32)

        def z_sends(parts):
            stack = jnp.stack(parts)
            return [pick(stack, pz ^ k, 0).astype(WIRE) for k in range(1, n_layers)], pick(stack, pz, 0)

        outs, sent = {}, {}
        layers = range(n_layers)

        def start(kind, l, msg, deps=()):
            if deps:
                msg = after(msg, deps)
            sent[kind, l] = swap(msg, 2 if l % 2 == 0 else 4)
            return msg

        def after_all(values, deps):
            return lax.optimization_barrier((tuple(values), *deps))[0]

        prev = ()

        def make(kind, l):
            nonlocal prev
            outs[kind, l] = product(kind, l, prev)
            msg = first_send(kind, l, outs[kind, l])
            prev = (msg,)
            return msg

        def sums(kind, ls, deps):
            got = after_all([sent[kind, l] for l in ls], deps)
            return [first_sum(kind, l, outs[kind, l], v) for l, v in zip(ls, got)]

        for l in layers:
            start("G", l, make("G", l))
        a_firsts = [make("A", l) for l in layers[:3]]
        firsts = sums("G", layers[:2], prev)
        g_msgs = [second_send(l, firsts[l]) for l in layers[:2]]
        prev = tuple(g_msgs)
        a_firsts.append(make("A", 3))
        s_firsts = [make("S", 3)]
        firsts += sums("G", layers[2:], prev)
        g_msgs += [second_send(l, firsts[l]) for l in layers[2:]]
        g_got = [swap(g_msgs[l], second_bit(l)) for l in layers]
        for l in layers:
            start("A", l, a_firsts[l], tuple(g_msgs))
        prev = tuple(g_msgs)
        s_firsts += [make("S", l) for l in (2, 1, 0)]
        for l, msg in zip((3, 2, 1, 0), s_firsts):
            start("S", l, msg, tuple(a_firsts + g_msgs))
        g_got = after_all(g_got, prev)
        sends, g_own = z_sends([second_sum(l, firsts[l], g_got[l]) for l in layers])
        for k, msg in enumerate(sends, 1):
            g_own = g_own + swap(msg, 8 * k).astype(jnp.float32)
        g_wire = g_own.astype(WIRE)
        g_from_x = swap(g_wire, 2)

        a_first = sums("A", layers, (g_wire,))
        a_msgs = [second_send(l, a_first[l]) for l in layers]
        a_got = [swap(a_msgs[l], second_bit(l)) for l in layers]
        g_x = ordered(g_wire, after(g_from_x, tuple(a_msgs)), 2, 0)
        g_from_y = swap(g_x, 4)
        s_first = sums("S", layers, (g_x,))
        s_msgs = [second_send(l, s_first[l]) for l in layers]
        s_got = [swap(s_msgs[l], second_bit(l)) for l in layers]
        g_y = ordered(g_x, after(g_from_y, tuple(s_msgs)), 4, 0).reshape(width, half)
        g_core = swap(g_y, 1)
        a_got = after_all(a_got, (g_y,))
        a_sends, a_total = z_sends([second_sum(l, a_first[l], a_got[l]) for l in layers])
        a_back = [swap(msg, 8 * k) for k, msg in enumerate(a_sends, 1)]

        other = after(g_core, tuple(a_sends))
        g_full = jnp.where(core == 0, jnp.concatenate([g_y, other], axis=1), jnp.concatenate([other, g_y], axis=1))
        g_full = after(g_full.astype(jnp.float32) * (unscale("G") / batch_total), ())
        left = jnp.dot(a_inv_rows, g_full, precision=PRECISE)
        u_rows = jnp.dot(after(left, ()), pick(s_inv, pz, 0), precision=PRECISE)
        e_u = exponent(jnp.max(jnp.abs(u_rows)))
        u_wire = fifth_power(u_rows * jnp.exp2(-e_u) * 2.0**20).astype(jnp.bfloat16)

        s_got = after_all(s_got, (u_wire,))
        s_sends, s_total = z_sends([second_sum(l, s_first[l], s_got[l]) for l in layers])
        s_back = [swap(msg, 8 * k) for k, msg in enumerate(s_sends, 1)]
        u_wire = after(u_wire, tuple(s_sends))
        u_all, e_all = spread(u_wire, jnp.broadcast_to(e_u, (8, 128)), n_dev)

        def finish(kind, old, back, total):
            for got in after_all(back, (e_all,)):
                total = total + got.astype(jnp.float32)
            got = swap(pick(total, 1 - core, 0), 1)
            keep = pick(total, core, 0)
            rows = jnp.where(core == 0, jnp.concatenate([keep, got], axis=1), jnp.concatenate([got, keep], axis=1))
            return FACTOR_DECAY * old + ((1.0 - FACTOR_DECAY) / batch_total) * (rows * unscale(kind))

        a_new = finish("A", a_old_rows, a_back, a_total)
        s_new = finish("S", s_old_rows, s_back, s_total)
        u_full = fifth_root(u_all.astype(jnp.float32)) * jnp.exp2(e_all[:, 0, 0] - 20.0)[:, None, None]
        return u_full.reshape(n_layers, width, width), a_new, s_new

    row_spec = P("data", None)
    return jax.shard_map(
        device_step,
        mesh=mesh,
        in_specs=(row_spec, row_spec, P(), row_spec, row_spec, row_spec, P()),
        out_specs=(P(), row_spec, row_spec),
        check_vma=False,
    )
```
